32 devices in a mesh: seq: 8 (over z, y), chan: 4 (over x, core).
Axes of the slice: x: 2, y: 2, z: 4, core: 2. Of those that a mesh axis runs over, the one named last changes fastest.
Arguments:
- inputs: float32 [1024, 8192], P('seq', 'chan'), may hold values from -6 to 6
- conv_weight: float32 [3, 4, 8192], P(None, None, 'chan'), may hold values from -3 to 3
- conv_bias: float32 [3, 8192], P(None, 'chan'), may hold values from -1 to 1
- cotangent: float32 [1024, 8192], P('seq', 'chan'), may hold values from -6 to 6
Outputs:
- output: float32 [1024, 8192], P('seq', 'chan')
- input_grad: float32 [1024, 8192], P('seq', 'chan')
- weight_grad: float32 [3, 4, 8192], P(None, None, 'chan')
- bias_grad: float32 [3, 8192], P(None, 'chan')
The draws below stay inside these ranges and needn't reach their ends.
All inputs are finite; a program needn't handle non-finite values.
Results may differ from the reference program's by a relative error of at most 0.0001.
Values sent between devices are 32-bit elements; how exact they have to be, the bound alone decides.
No kernel may reach another device: no remote copies, remote signals or barrier semaphores. Data moves between devices by JAX's collectives and lax.ppermute only.
A program may use at most 64 MiB of HBM per device.

```python
import jax
import jax.numpy as jnp

C = 8192
KW = 4
LAYERS = 3
TOKENS = 1024


def with_spikes(result, stream_key, source, target, shards_of, factor):
    owner, partner = [(jnp.arange(result.shape[position]) // (result.shape[position] // shards_of)).reshape([-1 if axis == position else 1 for axis in range(result.ndim)]) for position in (source, target)]
    chosen = jax.random.permutation(stream_key, shards_of)[partner]
    strong = (owner == chosen) | (owner == (partner + shards_of // 2) % shards_of)
    return jnp.where(strong, factor * result, result)


def shard_levels(key, extent, pieces, low, largest):
    loudness = 1.0
    for position, shards_of in pieces:
        heights = jax.random.uniform(jax.random.fold_in(jax.random.fold_in(key, 6), position), (shards_of,), jnp.float32, low / len(pieces), largest / len(pieces))
        loudness = loudness * jnp.repeat(jnp.exp(heights), extent[position] // shards_of).reshape((-1,) + (1,) * (len(extent) - 1 - position))
    return loudness


def noise(rng, dims, spread, bound, shards=(), kind=jnp.bfloat16):
    entries = jax.random.normal(rng, dims, jnp.float32) * spread
    if len(shards) > 0:
        entries = shard_levels(rng, dims, shards, -0.22, 0.18) * entries
    return jnp.clip(entries, min=-bound, max=bound).astype(kind)


def bell_draw_with(stream_key, shape, scale, most, pieces, heavy, kind=jnp.bfloat16):
    drawn = scale * jax.random.normal(stream_key, shape, jnp.float32)
    if pieces:
        drawn = drawn * shard_levels(stream_key, shape, pieces, -0.22, 0.18)
    return jnp.clip(with_spikes(drawn, jax.random.fold_in(stream_key, 3), *heavy), -most, most).astype(kind)


def setup_inputs(seed: int = 0) -> dict:
    streams_of = jax.random.split(jax.random.key(seed), 5)
    return {
        "inputs": noise(streams_of[0], (TOKENS, C), 1.0, 6.0, ((0, 8), (1, 4)), jnp.float32),
        "conv_weight": noise(streams_of[1], (LAYERS, KW, C), KW ** -0.5, 3.0, ((2, 4),), jnp.float32),
        "conv_bias": jnp.clip(jax.random.uniform(streams_of[2], (LAYERS, C), jnp.float32, -1.0, 1.0) * shard_levels(streams_of[2], (LAYERS, C), ((1, 4),), -0.4, 0.0), -1.0, 1.0),
        "cotangent": bell_draw_with(streams_of[3], (TOKENS, C), 1.0, 6.0, ((0, 8), (1, 4)), (0, 1, 8, 2.0), jnp.float32),
    }


def reference(inputs, conv_weight, conv_bias, cotangent):
    length = inputs.shape[0]
    act = inputs
    saved = []
    for layer in range(LAYERS):
        padded = jnp.pad(act, ((KW - 1, 0), (0, 0)))
        preact = conv_bias[layer][None, :] + sum(conv_weight[layer, offset][None, :] * padded[offset:offset + length] for offset in range(KW))
        saved.append((padded, preact))
        act = preact * jax.nn.sigmoid(preact)
    output = act
    grad = cotangent
    weight_list = [None] * LAYERS
    bias_list = [None] * LAYERS
    for layer in reversed(range(LAYERS)):
        padded, preact = saved[layer]
        gate_value = jax.nn.sigmoid(preact)
        pre_grad = grad * gate_value * (1.0 + preact * (1.0 - gate_value))
        grad_pad = jnp.pad(pre_grad, ((0, KW - 1), (0, 0)))
        grad = sum(conv_weight[layer, offset][None, :] * grad_pad[KW - 1 - offset:KW - 1 - offset + length] for offset in range(KW))
        weight_list[layer] = jnp.stack([jnp.sum(pre_grad * padded[offset:offset + length], axis=0) for offset in range(KW)])
        bias_list[layer] = jnp.sum(pre_grad, axis=0)
    return output, grad, jnp.stack(weight_list), jnp.stack(bias_list)
```

```python
import jax
import jax.numpy as jnp
from jax import lax
from jax.sharding import PartitionSpec as P


def passed_along(array, axis, by):
    devices = lax.axis_size(axis)
    pairs = [(i, i + by) for i in range(devices) if 0 <= i + by < devices]
    return lax.ppermute(array, axis, pairs)


def summed_over(array, axis):
    devices = lax.axis_size(axis)
    bit = 1
    while bit < devices:
        array = array + lax.ppermute(array, axis, [(i, i ^ bit) for i in range(devices)])
        bit *= 2
    return array


def shards(inputs, conv_weight, conv_bias, cotangent):
    n, width = inputs.shape
    layers, taps = conv_weight.shape[:2]
    reach = taps - 1
    halo = layers * reach
    packed = lambda a: a.reshape(a.shape[0], width // 128, 128)
    before = passed_along(packed(inputs[n - halo :]), "seq", 1).reshape(halo, width)
    after = passed_along(
        packed(jnp.concatenate([inputs[:halo], cotangent[:halo]], axis=0)), "seq", -1
    ).reshape(2 * halo, width)
    first = lax.axis_index("seq") == 0
    act = jnp.concatenate([before, inputs, after[:halo]], axis=0)
    grad = jnp.concatenate([cotangent, after[halo:]], axis=0)
    saved = []
    for layer in range(layers):
        rows = act.shape[0] - reach
        preact = conv_bias[layer][None, :] + sum(
            conv_weight[layer, k][None, :] * act[k : k + rows] for k in range(taps)
        )
        lead = halo - (layer + 1) * reach
        saved.append((act[lead : lead + reach + n], preact[lead:]))
        act = preact * jax.nn.sigmoid(preact)
        if lead:
            keep = jnp.logical_or(jnp.logical_not(first), jnp.arange(rows) >= lead)
            act = jnp.where(keep[:, None], act, 0.0)
    output = act[:n]
    terms = [None] * layers
    for layer in reversed(range(layers)):
        padded, preact = saved[layer]
        rows = grad.shape[0]
        gate = jax.nn.sigmoid(preact[:rows])
        pre_grad = grad * gate * (1.0 + preact[:rows] * (1.0 - gate))
        grad = sum(
            conv_weight[layer, k][None, :]
            * pre_grad[reach - k : reach - k + rows - reach]
            for k in range(taps)
        )
        own = pre_grad[:n]
        terms[layer] = jnp.stack(
            [jnp.sum(own * padded[k : k + n], axis=0) for k in range(taps)]
            + [jnp.sum(own, axis=0)]
        )
    total = summed_over(jnp.stack(terms).reshape(-1, 128), "seq")
    total = total.reshape(layers, taps + 1, width)
    return output, grad, total[:, :taps], total[:, taps]


def solution(mesh):
    in_specs = (P("seq", "chan"), P(None, None, "chan"), P(None, "chan"), P("seq", "chan"))
    out_specs = (P("seq", "chan"), P("seq", "chan"), P(None, None, "chan"), P(None, "chan"))
    return jax.shard_map(shards, mesh=mesh, in_specs=in_specs, out_specs=out_specs, check_vma=False)
```

```python
import functools

import jax
import jax.numpy as jnp
from jax import lax
from jax.experimental import pallas as pl
from jax.experimental.pallas import tpu as pltpu
from jax.sharding import PartitionSpec as P

LANES = 128
SUB = 8
BLOCK = 16


class Plan:
    def __init__(self, n, width, layers, taps):
        self.n, self.width, self.layers, self.taps = n, width, layers, taps
        self.reach = taps - 1
        self.halo = layers * self.reach
        self.cols = width // LANES
        self.groups = self.cols // SUB
        rows = []
        L, R, H = layers, self.reach, self.halo
        for l in range(1, L):
            rows += [("a", l, t) for t in range(l * R, H)]
            rows += [("a", l, t) for t in range(n - (L - l) * R, n)]
        for l in range(L - 1):
            rows += [("d", l, t) for t in range((l + 1) * R, H)]
            rows += [("d", l, t) for t in range(n - (L - 1 - l) * R, n)]
        for l in range(L):
            low = n - (L - 1 - l) * R
            rows += [("g", l, t) for t in range(H, H + R)]
            rows += [("g", l, t) for t in range(low - R, low)]
        top = -(-H // SUB) * SUB
        rows += [("out", 0, t) for t in range(H, top)]
        rows += [("grad", 0, t) for t in range(H, top)]
        rows += [("grad", 0, t) for t in range(n - top, n - H)]
        self.top = top
        self.state = {key: i for i, key in enumerate(rows)}
        self.acc = len(rows)
        self.state_rows = len(rows) + layers * (taps + 1)


def conv(weights, window):
    total = weights[0] * window[0]
    for k in range(1, len(window)):
        total = total + weights[k] * window[k]
    return total + weights[len(window)] if len(weights) > len(window) else total


def gate(h):
    u = jnp.tanh(h)
    v = 1.0 + u
    act = h * v
    return act, v + act * (1.0 - u)


def interior(p, x_ref, ct_ref, w_ref, b_ref, out_hbm, grad_hbm, st_ref, wb_ref, *scratch):
    L, R, H, K, n = p.layers, p.reach, p.halo, p.taps, p.n
    a_s, d_s = scratch[: L - 1], scratch[L - 1 : 2 * L - 1]
    g_s, out_s, grad_s, sem = scratch[2 * L - 1 :]
    blocks = n // BLOCK
    copies = []

    def send(src, dst, first, last, g, i):
        where = (pl.ds(first, last - first), pl.ds(g * SUB * SUB, SUB * SUB), slice(None))
        copies.append(pltpu.make_async_copy(src.at[where], dst.at[where], sem.at[i]))
        copies[-1].start()

    for l in range(L):
        for c in range(p.cols):
            wb_ref[l * (K + 1) + K, c : c + 1, :] = 0.5 * b_ref[l : l + 1, c * LANES : (c + 1) * LANES]
        for k in range(K):
            for g in range(p.groups):
                wb_ref[l * (K + 1) + k, g * SUB : (g + 1) * SUB, :] = 0.5 * w_ref[
                    pl.ds((l * p.cols + g * SUB) * K + k, SUB, stride=K), :
                ]

    for g in range(p.groups):
        lanes = pl.ds(g * SUB, SUB)

        def tile(ref, base, off):
            return (base // SUB + off // SUB, pl.ds(g * SUB * SUB + off % SUB, SUB, stride=SUB), slice(None))

        wb = [[wb_ref[l * (K + 1) + k, lanes, :] for k in range(K + 1)] for l in range(L)]

        def forward(base, windows, first):
            windows = [list(w) for w in windows]
            for off in range(BLOCK):
                act = x_ref[tile(x_ref, base, off)]
                for l in range(L):
                    windows[l] = windows[l] + [act]
                    if first and off < (l + 1) * R:
                        break
                    act, d = gate(conv(wb[l], windows[l][-K:]))
                    d_s[l][base + off, lanes, :] = d
                    if l < L - 1:
                        a_s[l][base + off, lanes, :] = act
                    else:
                        out_s[tile(out_s, base, off)] = act
            return [w[-R:] for w in windows]

        windows = forward(0, [[]] * L, True)
        lax.fori_loop(
            1, blocks, lambda i, w: forward(pl.multiple_of(i * BLOCK, BLOCK), w, False), windows
        )
        send(out_s, out_hbm, p.top // SUB, n // SUB, g, 3 * g)

        wt = [[wb_ref[l * (K + 1) + k, lanes, :] for k in range(K)] for l in range(L)]

        def backward(base, gs, acc, stop, last):
            gs, acc = [list(v) for v in gs], [list(v) for v in acc]
            acts = {}

            def act_at(l, off):
                if (l, off) not in acts:
                    if l == 0:
                        if off >= 0:
                            acts[l, off] = x_ref[tile(x_ref, base, off)]
                        else:
                            acts[l, off] = x_ref[tile(x_ref, base - BLOCK, off + BLOCK)]
                    else:
                        acts[l, off] = a_s[l - 1][base + off, lanes, :]
                return acts[l, off]

            for off in reversed(range(stop, BLOCK)):
                grad = ct_ref[tile(ct_ref, base, off)]
                for l in reversed(range(L)):
                    pre = grad * d_s[l][base + off, lanes, :]
                    gs[l] = ([pre] + gs[l])[:K]
                    for k in range(K):
                        acc[l][k] = acc[l][k] + pre * act_at(l, off - R + k)
                    acc[l][K] = acc[l][K] + pre
                    if not isinstance(base, int) or stop:
                        keep = stop and off < H + R
                    else:
                        keep = base + off < n - (L - 1 - l) * R and base + off >= n - (L - l) * R
                    if keep:
                        g_s[l, (base + off - (n - BLOCK)) if last else off, lanes, :] = pre
                    if last and base + off >= n - (L - l) * R:
                        break
                    grad = conv(wt[l][::-1], gs[l])
                else:
                    grad_s[tile(grad_s, base, off)] = grad
            return [v[:R] for v in gs], acc

        zero = jnp.zeros((SUB, LANES), jnp.float32)
        gs, acc = [[]] * L, [[zero] * (K + 1)] * L
        gs, acc = backward(n - BLOCK, gs, acc, 0, True)

        def keep_low():
            for l in range(L):
                low = n - (L - 1 - l) * R
                for t in range(low - R, low):
                    st_ref[p.state["g", l, t], lanes, :] = g_s[l, t - (n - BLOCK), lanes, :]

        keep_low()
        gs, acc = lax.fori_loop(
            0,
            blocks - 2,
            lambda i, c: backward(pl.multiple_of((blocks - 2 - i) * BLOCK, BLOCK), *c, 0, False),
            (gs, acc),
        )
        send(grad_s, grad_hbm, BLOCK // SUB, (n - p.top) // SUB, g, 3 * g + 1)
        gs, acc = backward(0, gs, acc, H, False)
        for l in range(L):
            for k in range(K + 1):
                st_ref[p.acc + l * (K + 1) + k, lanes, :] = acc[l][k]
        for (kind, l, t), i in p.state.items():
            if kind == "a":
                st_ref[i, lanes, :] = a_s[l - 1][t, lanes, :]
            elif kind == "d":
                st_ref[i, lanes, :] = d_s[l][t, lanes, :]
            elif kind == "g" and t < BLOCK:
                st_ref[i, lanes, :] = g_s[l, t, lanes, :]
            elif kind == "out":
                st_ref[i, lanes, :] = out_s[tile(out_s, 0, t)]
            elif kind == "grad":
                st_ref[i, lanes, :] = grad_s[tile(grad_s, 0, t)]
    for copy in copies:
        copy.wait()


def border(p, g, keep_ref, st_ref, wb_ref, xbot_ref, xtop_ref, ctop_ref, before_ref, after_ref, sums_ref, edge_ref):
    L, R, H, K, n = p.layers, p.reach, p.halo, p.taps, p.n
    lanes = pl.ds(g * SUB, SUB)
    wb = [[wb_ref[l * (K + 1) + k, lanes, :] for k in range(K + 1)] for l in range(L)]
    wt = [w[:K][::-1] for w in wb]
    acc = [[st_ref[p.acc + l * (K + 1) + k, lanes, :] for k in range(K + 1)] for l in range(L)]
    tiles = p.top // SUB
    state = lambda kind, l, t: st_ref[p.state[kind, l, t], lanes, :]

    def put(plane, t, value):
        edge_ref[plane * tiles + t // SUB, pl.ds(t % SUB, SUB, stride=SUB), :] = value

    def gather(l, pre, window):
        for k in range(K):
            acc[l][k] = acc[l][k] + pre * window[k]
        acc[l][K] = acc[l][K] + pre

    act = [dict() for _ in range(L + 1)]
    d = [dict() for _ in range(L)]
    pre = [dict() for _ in range(L)]
    for i in range(H):
        act[0][n - H + i] = xbot_ref[i, lanes, :]
        act[0][n + i] = after_ref[i, :, :]
    for l in range(1, L):
        for t in range(n - (L - l) * R, n):
            act[l][t] = state("a", l, t)
    for t in range(n, n + H):
        for l in range(L):
            a, dd = gate(conv(wb[l], [act[l][t - R + k] for k in range(K)]))
            act[l + 1][t] = a
            if t < n + (l + 1) * R:
                d[l][t] = dd
    grad = {t: after_ref[H + t - n, :, :] for t in range(n, n + H)}
    for l in reversed(range(L)):
        low = n - (L - 1 - l) * R
        for t in range(low - R, low):
            pre[l][t] = state("g", l, t)
        for t in grad:
            pre[l][t] = grad[t] * (d[l][t] if t >= n else state("d", l, t))
            if t < n:
                gather(l, pre[l][t], [act[l][t - R + k] for k in range(K)])
        high = n + (l + 1) * R
        grad = {t: conv(wt[l], [pre[l][t + k] for k in range(K)]) for t in range(low - R, high - R)}
    for t in range(n - p.top, n):
        put(2, t - (n - p.top), grad[t] if t in grad else state("grad", 0, t))

    keep = keep_ref[...]
    act = [dict() for _ in range(L + 1)]
    d = [dict() for _ in range(L)]
    for i in range(H):
        act[0][i - H] = before_ref[i, :, :]
        act[0][i] = xtop_ref[i, lanes, :]
    for l in range(L):
        for t in range(-(L - 1 - l) * R, (l + 1) * R):
            a, d[l][t] = gate(conv(wb[l], [act[l][t - R + k] for k in range(K)]))
            act[l + 1][t] = a * keep if t < 0 else a
        if l < L - 1:
            for t in range((l + 1) * R, H):
                act[l + 1][t] = state("a", l + 1, t)
                d[l][t] = state("d", l, t)
    for t in range(p.top):
        put(0, t, act[L][t] if t < H else state("out", 0, t))
    pre = [{t: state("g", l, t) for t in range(H, H + R)} for l in range(L)]
    for t in reversed(range(H)):
        grad = ctop_ref[t, lanes, :]
        for l in reversed(range(L)):
            pre[l][t] = grad * d[l][t]
            gather(l, pre[l][t], [act[l][t - R + k] for k in range(K)])
            grad = conv(wt[l], [pre[l][t + k] for k in range(K)])
        put(1, t, grad)
    for t in range(H, p.top):
        put(1, t, state("grad", 0, t))

    for l in range(L):
        for k in range(K):
            sums_ref[pl.ds(l * SUB * K + k, SUB, stride=K), :] = 0.5 * acc[l][k]
        sums_ref[pl.ds(L * SUB * K + l * SUB, SUB), :] = 0.5 * acc[l][K]


def edges(p, out_in, grad_in, *refs):
    edge_refs, (out_ref, grad_ref, sem) = refs[: p.groups], refs[p.groups :]
    tiles, size = p.top // SUB, SUB * SUB
    copies = []
    for g in range(p.groups):
        places = ((out_ref, 0), (grad_ref, 0), (grad_ref, p.n // SUB - tiles))
        for i, (ref, first) in enumerate(places):
            copies.append(
                pltpu.make_async_copy(
                    edge_refs[g].at[pl.ds(i * tiles, tiles)],
                    ref.at[pl.ds(first, tiles), pl.ds(g * size, size)],
                    sem.at[g * 3 + i],
                )
            )
    for copy in copies:
        copy.start()
    for copy in copies:
        copy.wait()


def passed_along(array, axis, by):
    devices = lax.axis_size(axis)
    pairs = [(i, i + by) for i in range(devices) if 0 <= i + by < devices]
    return lax.ppermute(array, axis, pairs)


def summed_over(array, axis):
    devices = lax.axis_size(axis)
    bit = 1
    while bit < devices:
        array = array + lax.ppermute(array, axis, [(i, i ^ bit) for i in range(devices)])
        bit *= 2
    return array


def tiled(a):
    n, width = a.shape
    return a.reshape(n // SUB, SUB, width // LANES, LANES).transpose(0, 2, 1, 3).reshape(n // SUB, -1, LANES)


def untiled(a, n, width):
    return a.reshape(n // SUB, width // LANES, SUB, LANES).transpose(0, 2, 1, 3).reshape(n, width)


def shards(inputs, conv_weight, conv_bias, cotangent):
    n, width = inputs.shape
    layers, taps = conv_weight.shape[:2]
    p = Plan(n, width, layers, taps)
    L, K, H, cols = layers, taps, p.halo, p.cols
    f32 = lambda *shape: jax.ShapeDtypeStruct(shape, jnp.float32)
    vmem, hbm = pl.BlockSpec(memory_space=pltpu.VMEM), pl.BlockSpec(memory_space=pltpu.HBM)

    rowed = lambda a: a.reshape(a.shape[0], cols, LANES)
    xbot, xtop, ctop = rowed(inputs[n - H :]), rowed(inputs[:H]), rowed(cotangent[:H])
    part = lambda a, g: a[:, g * SUB : (g + 1) * SUB]
    befores, afters = [], []
    for g in range(p.groups):
        befores.append(passed_along(part(xbot, g), "seq", 1))
        afters.append(passed_along(jnp.concatenate([part(xtop, g), part(ctop, g)], axis=0), "seq", -1))

    weights = conv_weight.reshape(L, K, cols, LANES).transpose(0, 2, 1, 3).reshape(L * cols * K, LANES)
    shape = (n // SUB, cols * SUB, LANES)
    per_row = (n, cols, LANES)
    work = n * width
    out, grad, st, wb = pl.pallas_call(
        functools.partial(interior, p),
        out_shape=(f32(*shape), f32(*shape), f32(p.state_rows, cols, LANES), f32(L * (K + 1), cols, LANES)),
        in_specs=[vmem] * 4,
        out_specs=(hbm, hbm, vmem, vmem),
        scratch_shapes=[pltpu.VMEM(per_row, jnp.float32)] * (2 * L - 1)
        + [pltpu.VMEM((L, BLOCK, cols, LANES), jnp.float32)]
        + [pltpu.VMEM(shape, jnp.float32)] * 2
        + [pltpu.SemaphoreType.DMA((3 * p.groups,))],
        compiler_params=pltpu.CompilerParams(vmem_limit_bytes=24 << 20),
        cost_estimate=pl.CostEstimate(flops=90 * work, bytes_accessed=16 * work, transcendentals=L * work),
        name="interior",
    )(tiled(inputs), tiled(cotangent), weights, conv_bias)

    keep = jnp.where(lax.axis_index("seq") == 0, 0.0, 1.0) * jnp.ones((SUB, LANES), jnp.float32)
    tiles = 3 * p.top // SUB
    totals, edge = [], []
    for g in range(p.groups):
        sums, e = pl.pallas_call(
            functools.partial(border, p, g),
            out_shape=(f32(L * (K + 1) * SUB, LANES), f32(tiles, SUB * SUB, LANES)),
            in_specs=[vmem] * 8,
            out_specs=(vmem, vmem),
            compiler_params=pltpu.CompilerParams(vmem_limit_bytes=8 << 20),
            cost_estimate=pl.CostEstimate(flops=10 * work, bytes_accessed=0, transcendentals=0),
            name=f"border{g}",
        )(keep, st, wb, xbot, xtop, ctop, befores[g], afters[g])
        totals.append(summed_over(sums, "seq"))
        edge.append(e)

    out, grad = pl.pallas_call(
        functools.partial(edges, p),
        out_shape=(f32(*shape), f32(*shape)),
        in_specs=[hbm, hbm] + [vmem] * p.groups,
        out_specs=(hbm, hbm),
        scratch_shapes=[pltpu.SemaphoreType.DMA((3 * p.groups,))],
        input_output_aliases={0: 0, 1: 1},
        compiler_params=pltpu.CompilerParams(vmem_limit_bytes=4 << 20),
        cost_estimate=pl.CostEstimate(flops=5 * work, bytes_accessed=0, transcendentals=0),
        name="edges",
    )(out, grad, *edge)

    cut = L * SUB * K
    w_sum = jnp.concatenate([t[:cut].reshape(L, SUB, K, LANES) for t in totals], axis=1)
    b_sum = jnp.concatenate([t[cut:].reshape(L, SUB, LANES) for t in totals], axis=1)
    return (
        untiled(out, n, width),
        untiled(grad, n, width),
        w_sum.transpose(0, 2, 1, 3).reshape(L, K, width),
        b_sum.reshape(L, width),
    )


def solution(mesh):
    in_specs = (P("seq", "chan"), P(None, None, "chan"), P(None, "chan"), P("seq", "chan"))
    out_specs = (P("seq", "chan"), P("seq", "chan"), P(None, None, "chan"), P(None, "chan"))
    return jax.shard_map(shards, mesh=mesh, in_specs=in_specs, out_specs=out_specs, check_vma=False)
```

```python
import functools

import jax
import jax.numpy as jnp
from jax import lax
from jax.experimental import pallas as pl
from jax.experimental.pallas import tpu as pltpu
from jax.sharding import PartitionSpec as P

LANES = 128
SUB = 8
BLOCK = 16


class Plan:
    def __init__(self, n, width, layers, taps):
        self.n, self.width, self.layers, self.taps = n, width, layers, taps
        self.reach = taps - 1
        self.halo = layers * self.reach
        self.late = self.halo - self.reach
        self.cols = width // LANES
        self.groups = self.cols // SUB
        self.top = top = -(-self.halo // SUB) * SUB
        rows = []
        L, R, H = layers, self.reach, self.halo
        rows += [(kind, 0, t) for kind in ("x", "ct") for t in range(H)]
        for l in range(1, L):
            rows += [("a", l, t) for t in range(l * R, H)]
        for l in range(L - 1):
            rows += [("d", l, t) for t in range((l + 1) * R, H)]
            rows += [("d", l, t) for t in range(n - (L - 1 - l) * R, n)]
        for l in range(L):
            low = n - (L - 1 - l) * R
            rows += [("g", l, t) for t in range(H, H + R)]
            rows += [("g", l, t) for t in range(low - R, low)]
        rows += [("out", 0, t) for t in range(H, top)]
        rows += [("grad", 0, t) for t in range(H, top)]
        rows += [("grad", 0, t) for t in range(n - top, n - H)]
        self.state = {key: i for i, key in enumerate(rows)}
        self.acc = len(rows)
        self.state_rows = len(rows) + layers * (taps + 1)


def conv(weights, window):
    total = weights[0] * window[0]
    for k in range(1, len(window)):
        total = total + weights[k] * window[k]
    return total + weights[len(window)] if len(weights) > len(window) else total


def gate(h):
    u = jnp.tanh(h)
    v = 1.0 + u
    act = h * v
    return act, v + act * (1.0 - u)


def interior(p, x_ref, ct_ref, w_ref, b_ref, out_hbm, grad_hbm, st_ref, wb_ref, *scratch):
    L, R, H, K, n = p.layers, p.reach, p.halo, p.taps, p.n
    a_s, d_s = scratch[: L - 1], scratch[L - 1 : 2 * L - 1]
    out_s, grad_s, sem = scratch[2 * L - 1 :]
    blocks = n // BLOCK
    copies = []

    def send(src, dst, first, last, g, i):
        where = (pl.ds(first, last - first), pl.ds(g * SUB * SUB, SUB * SUB), slice(None))
        copies.append(pltpu.make_async_copy(src.at[where], dst.at[where], sem.at[i]))
        copies[-1].start()

    for l in range(L):
        for g in range(p.groups):
            for k in range(K):
                wb_ref[l * (K + 1) + k, g * SUB : (g + 1) * SUB, :] = 0.5 * w_ref[
                    pl.ds((l * p.cols + g * SUB) * K + k, SUB, stride=K), :
                ]
            wb_ref[l * (K + 1) + K, g * SUB : (g + 1) * SUB, :] = 0.5 * b_ref[l, g * SUB : (g + 1) * SUB, :]

    for g in range(p.groups):
        lanes = pl.ds(g * SUB, SUB)

        def tile(base, off):
            return (base // SUB + off // SUB, pl.ds(g * SUB * SUB + off % SUB, SUB, stride=SUB), slice(None))

        wb = [[wb_ref[l * (K + 1) + k, lanes, :] for k in range(K + 1)] for l in range(L)]

        def forward(base, windows, first):
            windows = [list(w) for w in windows]
            for off in range(BLOCK):
                act = x_ref[tile(base, off)]
                for l in range(L):
                    windows[l] = windows[l] + [act]
                    if first and off < (l + 1) * R:
                        break
                    act, d = gate(conv(wb[l], windows[l][-K:]))
                    d_s[l][base + off, lanes, :] = d
                    if l < L - 1:
                        a_s[l][base + off, lanes, :] = act
                    else:
                        out_s[tile(base, off)] = act
            return [w[-R:] for w in windows]

        windows = forward(0, [[]] * L, True)
        lax.fori_loop(
            1, blocks, lambda i, w: forward(pl.multiple_of(i * BLOCK, BLOCK), w, False), windows
        )
        send(out_s, out_hbm, p.top // SUB, n // SUB, g, 3 * g)

        wt = [[wb_ref[l * (K + 1) + k, lanes, :] for k in range(K)] for l in range(L)]

        def backward(base, gs, acc, stop, last):
            gs, acc = [list(v) for v in gs], [list(v) for v in acc]
            acts = {}

            def act_at(l, off):
                if (l, off) not in acts:
                    if l == 0:
                        if off >= 0:
                            acts[l, off] = x_ref[tile(base, off)]
                        else:
                            acts[l, off] = x_ref[tile(base - BLOCK, off + BLOCK)]
                    else:
                        acts[l, off] = a_s[l - 1][base + off, lanes, :]
                return acts[l, off]

            for off in reversed(range(stop, BLOCK)):
                grad = ct_ref[tile(base, off)]
                for l in reversed(range(L)):
                    pre = grad * d_s[l][base + off, lanes, :]
                    gs[l] = ([pre] + gs[l])[:K]
                    for k in range(K):
                        acc[l][k] = acc[l][k] + pre * act_at(l, off - R + k)
                    acc[l][K] = acc[l][K] + pre
                    key = ("g", l, base + off if last or stop else None)
                    if key in p.state:
                        st_ref[p.state[key], lanes, :] = pre
                    if last and base + off >= n - (L - l) * R:
                        break
                    grad = conv(wt[l][::-1], gs[l])
                else:
                    grad_s[tile(base, off)] = grad
            return [v[:R] for v in gs], acc

        zero = jnp.zeros((SUB, LANES), jnp.float32)
        gs, acc = [[]] * L, [[zero] * (K + 1)] * L
        gs, acc = backward(n - BLOCK, gs, acc, 0, True)

        gs, acc = lax.fori_loop(
            0,
            blocks - 2,
            lambda i, c: backward(pl.multiple_of((blocks - 2 - i) * BLOCK, BLOCK), *c, 0, False),
            (gs, acc),
        )
        send(grad_s, grad_hbm, BLOCK // SUB, (n - p.top) // SUB, g, 3 * g + 1)
        gs, acc = backward(0, gs, acc, H, False)
        for l in range(L):
            for k in range(K + 1):
                st_ref[p.acc + l * (K + 1) + k, lanes, :] = acc[l][k]
        for (kind, l, t), i in p.state.items():
            if kind == "a":
                st_ref[i, lanes, :] = a_s[l - 1][t, lanes, :]
            elif kind == "d":
                st_ref[i, lanes, :] = d_s[l][t, lanes, :]
            elif kind == "x":
                st_ref[i, lanes, :] = x_ref[tile(0, t)]
            elif kind == "ct":
                st_ref[i, lanes, :] = ct_ref[tile(0, t)]
            elif kind == "out":
                st_ref[i, lanes, :] = out_s[tile(0, t)]
            elif kind == "grad":
                st_ref[i, lanes, :] = grad_s[tile(0, t)]
    for copy in copies:
        copy.wait()


def border(p, keep_ref, st_ref, wb_ref, up_ref, edge_ref, ret_ref, sums_ref):
    L, R, H, K, M = p.layers, p.reach, p.halo, p.taps, p.late
    size = L * (K + 1) * SUB
    tiles = p.top // SUB
    keep = keep_ref[...]
    for g in range(p.groups):
        lanes = pl.ds(g * SUB, SUB)
        wb = [[wb_ref[l * (K + 1) + k, lanes, :] for k in range(K + 1)] for l in range(L)]
        wt = [w[:K][::-1] for w in wb]
        acc = [[st_ref[p.acc + l * (K + 1) + k, lanes, :] for k in range(K + 1)] for l in range(L)]
        state = lambda kind, l, t: st_ref[p.state[kind, l, t], lanes, :]

        def put(plane, t, value):
            where = (plane * tiles + t // SUB, pl.ds(g * SUB * SUB + t % SUB, SUB, stride=SUB), slice(None))
            edge_ref[where] = value

        act = [dict() for _ in range(L + 1)]
        kept = [dict() for _ in range(L + 1)]
        d = [dict() for _ in range(L)]
        for t in range(-M - H, H):
            act[0][t] = up_ref[M + H + t, lanes, :] if t < 0 else state("x", 0, t)

        def past(l, t):
            rows = range(t - R, t + 1)
            if t < 0:
                return [act[l][s] for s in rows]
            return [kept[l][s] if s < 0 else act[l][s] for s in rows]

        for l in range(L):
            for t in range(-R, 0):
                kept[l][t] = act[l][t] * keep
            for t in range(-M - H + (l + 1) * R, (l + 1) * R):
                act[l + 1][t], d[l][t] = gate(conv(wb[l], past(l, t)))
            if l < L - 1:
                for t in range((l + 1) * R, H):
                    act[l + 1][t], d[l][t] = state("a", l + 1, t), state("d", l, t)
        for t in range(p.top):
            put(0, t, act[L][t] if t < H else state("out", 0, t))

        pre = [{t: state("g", l, t) for t in range(H, H + R)} for l in range(L)]
        for t in reversed(range(-M, H)):
            if t == -1:
                for l in range(L):
                    for s in range(R):
                        pre[l][s] = ret_ref[l * R + s, lanes, :]
            grad = up_ref[2 * M + H + t, lanes, :] if t < 0 else state("ct", 0, t)
            for l in reversed(range(L)):
                pre[l][t] = grad * d[l][t]
                if 0 <= t < R:
                    ret_ref[l * R + t, lanes, :] = pre[l][t] * keep
                if t >= -(L - 1 - l) * R:
                    window = past(l, t)
                    for k in range(K):
                        acc[l][k] = acc[l][k] + pre[l][t] * window[k]
                    acc[l][K] = acc[l][K] + pre[l][t]
                if t >= 0 or l > 0:
                    grad = conv(wt[l], [pre[l][t + k] for k in range(K)])
            if t >= 0:
                put(1, t, grad)
        for t in range(H, p.top):
            put(1, t, state("grad", 0, t))

        for l in range(L):
            for k in range(K):
                sums_ref[pl.ds(g * size + l * SUB * K + k, SUB, stride=K), :] = 0.5 * acc[l][k]
            sums_ref[pl.ds(g * size + L * SUB * K + l * SUB, SUB), :] = 0.5 * acc[l][K]


def edges(p, out_in, grad_in, edge_ref, st_ref, wb_ref, ret_ref, out_ref, grad_ref, low_s, sem):
    tiles, L, R, H, K, n = p.top // SUB, p.layers, p.reach, p.halo, p.taps, p.n
    copies = [
        pltpu.make_async_copy(edge_ref.at[pl.ds(0, tiles)], out_ref.at[pl.ds(0, tiles)], sem.at[0]),
        pltpu.make_async_copy(edge_ref.at[pl.ds(tiles, tiles)], grad_ref.at[pl.ds(0, tiles)], sem.at[1]),
        pltpu.make_async_copy(low_s, grad_ref.at[pl.ds(n // SUB - tiles, tiles)], sem.at[2]),
    ]
    copies[0].start()
    copies[1].start()
    for g in range(p.groups):
        lanes = pl.ds(g * SUB, SUB)
        state = lambda kind, l, t: st_ref[p.state[kind, l, t], lanes, :]
        grad = {}
        for l in reversed(range(L)):
            wt = [wb_ref[l * (K + 1) + k, lanes, :] for k in reversed(range(K))]
            low = n - (L - 1 - l) * R
            pre = {n + s: ret_ref[l * R + s, lanes, :] for s in range(R)}
            for t in range(low - R, n):
                pre[t] = grad[t] * state("d", l, t) if t >= low else state("g", l, t)
            grad = {t: conv(wt, [pre[t + k] for k in range(K)]) for t in range(low - R, n)}
        for i in range(p.top):
            t = n - p.top + i
            row = grad[t] if t in grad else state("grad", 0, t)
            low_s[i // SUB, pl.ds(g * SUB * SUB + i % SUB, SUB, stride=SUB), :] = row
    copies[2].start()
    for copy in copies:
        copy.wait()


def finish(p, mine_ref, theirs_ref, w_ref, b_ref):
    L, K = p.layers, p.taps
    size = L * (K + 1) * SUB
    for g in range(p.groups):
        for l in range(L):
            for rows, where in ((SUB * K, l * SUB * K), (SUB, L * SUB * K + l * SUB)):
                there = pl.ds(g * size + where, rows)
                total = mine_ref[there, :] + theirs_ref[there, :]
                if rows == SUB * K:
                    w_ref[pl.ds((l * p.cols + g * SUB) * K, rows), :] = total
                else:
                    for c in range(SUB):
                        at = (g * SUB + c) * LANES
                        b_ref[l : l + 1, at : at + LANES] = total[c : c + 1, :]


def shifted(array, axis, by):
    devices = lax.axis_size(axis)
    return lax.ppermute(array, axis, [(i, (i + by) % devices) for i in range(devices)])


def swapped(array, axis, bit):
    return lax.ppermute(array, axis, [(i, i ^ bit) for i in range(lax.axis_size(axis))])


def summed_but_one(array, axis):
    devices = lax.axis_size(axis)
    bits = [1 << i for i in range(devices.bit_length() - 1)]
    if len(bits) > 2:
        one, two = bits[:2]
        near, far, both = [swapped(array, axis, bit) for bit in (one, two, one ^ two)]
        array = (array + near) + (far + both)
        bits = bits[2:]
    for bit in bits[:-1]:
        array = array + swapped(array, axis, bit)
    return array, swapped(array, axis, bits[-1])


def tiled(a):
    n, width = a.shape
    return a.reshape(n // SUB, SUB, width // LANES, LANES).transpose(0, 2, 1, 3).reshape(n // SUB, -1, LANES)


def untiled(a, n, width):
    return a.reshape(n // SUB, width // LANES, SUB, LANES).transpose(0, 2, 1, 3).reshape(n, width)


def shards(inputs, conv_weight, conv_bias, cotangent):
    n, width = inputs.shape
    layers, taps = conv_weight.shape[:2]
    p = Plan(n, width, layers, taps)
    L, K, H, cols = layers, taps, p.halo, p.cols
    f32 = lambda *shape: jax.ShapeDtypeStruct(shape, jnp.float32)
    vmem, hbm = pl.BlockSpec(memory_space=pltpu.VMEM), pl.BlockSpec(memory_space=pltpu.HBM)

    shape = (n // SUB, cols * SUB, LANES)
    per_row = (n, cols, LANES)
    work = n * width
    cost = lambda flops: pl.CostEstimate(flops=flops * work, bytes_accessed=0, transcendentals=0)
    params = lambda mib: pltpu.CompilerParams(vmem_limit_bytes=mib << 20)
    x, ct = tiled(inputs), tiled(cotangent)
    weights = conv_weight.reshape(L, K, cols, LANES).transpose(0, 2, 1, 3).reshape(L * cols * K, LANES)

    M = p.late
    rows = jnp.concatenate([inputs[n - M - H :], cotangent[n - M :], conv_bias], axis=0).reshape(-1, cols, LANES)
    from_before = shifted(rows[: 2 * M + H], "seq", 1)

    out, grad, st, wb = pl.pallas_call(
        functools.partial(interior, p),
        out_shape=(f32(*shape), f32(*shape), f32(p.state_rows, cols, LANES), f32(L * (K + 1), cols, LANES)),
        in_specs=[vmem] * 4,
        out_specs=(hbm, hbm, vmem, vmem),
        scratch_shapes=[pltpu.VMEM(per_row, jnp.float32)] * (2 * L - 1)
        + [pltpu.VMEM(shape, jnp.float32)] * 2
        + [pltpu.SemaphoreType.DMA((3 * p.groups,))],
        compiler_params=params(24),
        cost_estimate=cost(90),
        name="interior",
    )(x, ct, weights, rows[2 * M + H :])

    keep = jnp.where(lax.axis_index("seq") == 0, 0.0, 1.0) * jnp.ones((SUB, LANES), jnp.float32)
    edge, ret, sums = pl.pallas_call(
        functools.partial(border, p),
        out_shape=(
            f32(2 * p.top // SUB, *shape[1:]),
            f32(H, cols, LANES),
            f32(L * (K + 1) * cols, LANES),
        ),
        in_specs=[vmem] * 4,
        out_specs=(vmem,) * 3,
        compiler_params=params(8),
        cost_estimate=cost(10),
        name="border",
    )(keep, st, wb, from_before)
    mine, theirs = summed_but_one(sums, "seq")
    returned = shifted(ret, "seq", -1)

    out, grad = pl.pallas_call(
        functools.partial(edges, p),
        out_shape=(f32(*shape), f32(*shape)),
        in_specs=[hbm, hbm] + [vmem] * 4,
        out_specs=(hbm, hbm),
        scratch_shapes=[
            pltpu.VMEM((p.top // SUB, *shape[1:]), jnp.float32),
            pltpu.SemaphoreType.DMA((3,)),
        ],
        input_output_aliases={0: 0, 1: 1},
        compiler_params=params(4),
        cost_estimate=cost(5),
        name="edges",
    )(out, grad, edge, st, wb, returned)

    w_sum, b_sum = pl.pallas_call(
        functools.partial(finish, p),
        out_shape=(f32(*weights.shape), f32(L, width)),
        in_specs=[vmem] * 2,
        out_specs=(vmem, vmem),
        compiler_params=params(4),
        cost_estimate=cost(5),
        name="finish",
    )(mine, theirs)
    return (
        untiled(out, n, width),
        untiled(grad, n, width),
        w_sum.reshape(L, cols, K, LANES).transpose(0, 2, 1, 3).reshape(L, K, width),
        b_sum,
    )


def solution(mesh):
    in_specs = (P("seq", "chan"), P(None, None, "chan"), P(None, "chan"), P("seq", "chan"))
    out_specs = (P("seq", "chan"), P("seq", "chan"), P(None, None, "chan"), P(None, "chan"))
    return jax.shard_map(shards, mesh=mesh, in_specs=in_specs, out_specs=out_specs, check_vma=False)
```

```python
import functools

import jax
import jax.numpy as jnp
from jax import lax
from jax.experimental import pallas as pl
from jax.experimental.pallas import tpu as pltpu
from jax.sharding import PartitionSpec as P


LANES = 128
SUB = 8
BLOCK = 16


class Plan:
    def __init__(self, n, width, layers, taps):
        self.n, self.width, self.layers, self.taps = n, width, layers, taps
        self.reach = taps - 1
        self.halo = layers * self.reach
        self.late = self.halo - self.reach
        self.cols = width // LANES
        self.groups = self.cols // SUB
        self.top = top = -(-self.halo // SUB) * SUB
        rows = []
        L, R, H = layers, self.reach, self.halo
        rows += [(kind, 0, t) for kind in ("x", "ct") for t in range(H)]
        for l in range(1, L):
            rows += [("a", l, t) for t in range(l * R, H)]
        for l in range(L - 1):
            rows += [("d", l, t) for t in range((l + 1) * R, H)]
            rows += [("d", l, t) for t in range(n - (L - 1 - l) * R, n)]
        for l in range(L):
            low = n - (L - 1 - l) * R
            rows += [("g", l, t) for t in range(H, H + R)]
            rows += [("g", l, t) for t in range(low - R, low)]
        rows += [("out", 0, t) for t in range(H, top)]
        rows += [("grad", 0, t) for t in range(H, top)]
        rows += [("grad", 0, t) for t in range(n - top, n - H)]
        self.state = {key: i for i, key in enumerate(rows)}
        self.acc = len(rows)
        self.state_rows = len(rows) + layers * (taps + 1)


def conv(weights, window):
    total = weights[0] * window[0]
    for k in range(1, len(window)):
        total = total + weights[k] * window[k]
    return total + weights[len(window)] if len(weights) > len(window) else total


def gate(h):
    u = jnp.tanh(h)
    v = 1.0 + u
    act = h * v
    return act, v + act * (1.0 - u)


def interior(p, x_ref, ct_ref, w_ref, b_ref, out_hbm, grad_hbm, st_ref, wb_ref, *scratch):
    L, R, H, K, n = p.layers, p.reach, p.halo, p.taps, p.n
    a_s, d_s = scratch[: L - 1], scratch[L - 1 : 2 * L - 1]
    out_s, grad_s, sem = scratch[2 * L - 1 :]
    blocks = n // BLOCK
    copies = []

    def send(src, dst, first, last, g, i):
        where = (pl.ds(first, last - first), pl.ds(g * SUB * SUB, SUB * SUB), slice(None))
        copies.append(pltpu.make_async_copy(src.at[where], dst.at[where], sem.at[i]))
        copies[-1].start()

    for l in range(L):
        for g in range(p.groups):
            for k in range(K):
                wb_ref[l * (K + 1) + k, g * SUB : (g + 1) * SUB, :] = 0.5 * w_ref[
                    pl.ds((l * p.cols + g * SUB) * K + k, SUB, stride=K), :
                ]
            wb_ref[l * (K + 1) + K, g * SUB : (g + 1) * SUB, :] = 0.5 * b_ref[l, g * SUB : (g + 1) * SUB, :]

    for g in range(p.groups):
        lanes = pl.ds(g * SUB, SUB)

        def tile(base, off):
            return (base // SUB + off // SUB, pl.ds(g * SUB * SUB + off % SUB, SUB, stride=SUB), slice(None))

        wb = [[wb_ref[l * (K + 1) + k, lanes, :] for k in range(K + 1)] for l in range(L)]

        def forward(base, windows, first):
            windows = [list(w) for w in windows]
            for off in range(BLOCK):
                act = x_ref[tile(base, off)]
                for l in range(L):
                    windows[l] = windows[l] + [act]
                    if first and off < (l + 1) * R:
                        break
                    act, d = gate(conv(wb[l], windows[l][-K:]))
                    d_s[l][base + off, lanes, :] = d
                    if l < L - 1:
                        a_s[l][base + off, lanes, :] = act
                    else:
                        out_s[tile(base, off)] = act
            return [w[-R:] for w in windows]

        windows = forward(0, [[]] * L, True)
        lax.fori_loop(
            1, blocks, lambda i, w: forward(pl.multiple_of(i * BLOCK, BLOCK), w, False), windows
        )
        send(out_s, out_hbm, p.top // SUB, n // SUB, g, 3 * g)

        wt = [[wb_ref[l * (K + 1) + k, lanes, :] for k in range(K)] for l in range(L)]

        def backward(base, gs, acc, stop, last):
            gs, acc = [list(v) for v in gs], [list(v) for v in acc]
            acts = {}

            def act_at(l, off):
                if (l, off) not in acts:
                    if l == 0:
                        if off >= 0:
                            acts[l, off] = x_ref[tile(base, off)]
                        else:
                            acts[l, off] = x_ref[tile(base - BLOCK, off + BLOCK)]
                    else:
                        acts[l, off] = a_s[l - 1][base + off, lanes, :]
                return acts[l, off]

            for off in reversed(range(stop, BLOCK)):
                grad = ct_ref[tile(base, off)]
                for l in reversed(range(L)):
                    pre = grad * d_s[l][base + off, lanes, :]
                    gs[l] = ([pre] + gs[l])[:K]
                    for k in range(K):
                        acc[l][k] = acc[l][k] + pre * act_at(l, off - R + k)
                    acc[l][K] = acc[l][K] + pre
                    key = ("g", l, base + off if last or stop else None)
                    if key in p.state:
                        st_ref[p.state[key], lanes, :] = pre
                    if last and base + off >= n - (L - l) * R:
                        break
                    grad = conv(wt[l][::-1], gs[l])
                else:
                    grad_s[tile(base, off)] = grad
            return [v[:R] for v in gs], acc

        zero = jnp.zeros((SUB, LANES), jnp.float32)
        gs, acc = [[]] * L, [[zero] * (K + 1)] * L
        gs, acc = backward(n - BLOCK, gs, acc, 0, True)

        gs, acc = lax.fori_loop(
            0,
            blocks - 2,
            lambda i, c: backward(pl.multiple_of((blocks - 2 - i) * BLOCK, BLOCK), *c, 0, False),
            (gs, acc),
        )
        send(grad_s, grad_hbm, BLOCK // SUB, (n - p.top) // SUB, g, 3 * g + 1)
        gs, acc = backward(0, gs, acc, H, False)
        for l in range(L):
            for k in range(K + 1):
                st_ref[p.acc + l * (K + 1) + k, lanes, :] = acc[l][k]
        for (kind, l, t), i in p.state.items():
            if kind == "a":
                st_ref[i, lanes, :] = a_s[l - 1][t, lanes, :]
            elif kind == "d":
                st_ref[i, lanes, :] = d_s[l][t, lanes, :]
            elif kind == "x":
                st_ref[i, lanes, :] = x_ref[tile(0, t)]
            elif kind == "ct":
                st_ref[i, lanes, :] = ct_ref[tile(0, t)]
            elif kind == "out":
                st_ref[i, lanes, :] = out_s[tile(0, t)]
            elif kind == "grad":
                st_ref[i, lanes, :] = grad_s[tile(0, t)]
    for copy in copies:
        copy.wait()


def border(p, keep_ref, st_ref, wb_ref, up_ref, edge_ref, ret_ref, sums_ref):
    L, R, H, K, M = p.layers, p.reach, p.halo, p.taps, p.late
    size = L * (K + 1) * SUB
    tiles = p.top // SUB
    keep = keep_ref[...]
    for g in range(p.groups):
        lanes = pl.ds(g * SUB, SUB)
        wb = [[wb_ref[l * (K + 1) + k, lanes, :] for k in range(K + 1)] for l in range(L)]
        wt = [w[:K][::-1] for w in wb]
        acc = [[st_ref[p.acc + l * (K + 1) + k, lanes, :] for k in range(K + 1)] for l in range(L)]
        state = lambda kind, l, t: st_ref[p.state[kind, l, t], lanes, :]

        def put(plane, t, value):
            where = (plane * tiles + t // SUB, pl.ds(g * SUB * SUB + t % SUB, SUB, stride=SUB), slice(None))
            edge_ref[where] = value

        act = [dict() for _ in range(L + 1)]
        kept = [dict() for _ in range(L + 1)]
        d = [dict() for _ in range(L)]
        for t in range(-M - H, H):
            act[0][t] = up_ref[up_ref.shape[0] + t, lanes, :] if t < 0 else state("x", 0, t)

        def past(l, t):
            rows = range(t - R, t + 1)
            if t < 0:
                return [act[l][s] for s in rows]
            return [kept[l][s] if s < 0 else act[l][s] for s in rows]

        for l in range(L):
            for t in range(-R, 0):
                kept[l][t] = act[l][t] * keep
            for t in range(-M - H + (l + 1) * R, (l + 1) * R):
                act[l + 1][t], d[l][t] = gate(conv(wb[l], past(l, t)))
            if l < L - 1:
                for t in range((l + 1) * R, H):
                    act[l + 1][t], d[l][t] = state("a", l + 1, t), state("d", l, t)
        for t in range(p.top):
            put(0, t, act[L][t] if t < H else state("out", 0, t))

        pre = [{t: state("g", l, t) for t in range(H, H + R)} for l in range(L)]
        for t in reversed(range(-M, H)):
            if t == -1:
                for l in range(L):
                    for s in range(R):
                        pre[l][s] = ret_ref[l * R + s, lanes, :]
            grad = up_ref[M + t, lanes, :] if t < 0 else state("ct", 0, t)
            for l in reversed(range(L)):
                pre[l][t] = grad * d[l][t]
                if 0 <= t < R:
                    ret_ref[l * R + t, lanes, :] = pre[l][t] * keep
                if t >= -(L - 1 - l) * R:
                    window = past(l, t)
                    for k in range(K):
                        acc[l][k] = acc[l][k] + pre[l][t] * window[k]
                    acc[l][K] = acc[l][K] + pre[l][t]
                if t >= 0 or l > 0:
                    grad = conv(wt[l], [pre[l][t + k] for k in range(K)])
            if t >= 0:
                put(1, t, grad)
        for t in range(H, p.top):
            put(1, t, state("grad", 0, t))

        for l in range(L):
            for k in range(K):
                sums_ref[pl.ds(g * size + l * SUB * K + k, SUB, stride=K), :] = 0.5 * acc[l][k]
            sums_ref[pl.ds(g * size + L * SUB * K + l * SUB, SUB), :] = 0.5 * acc[l][K]


def edges(p, out_in, grad_in, edge_ref, st_ref, wb_ref, ret_ref, out_ref, grad_ref, low_s, sem):
    tiles, L, R, K, n = p.top // SUB, p.layers, p.reach, p.taps, p.n
    copies = [
        pltpu.make_async_copy(edge_ref.at[pl.ds(0, tiles)], out_ref.at[pl.ds(0, tiles)], sem.at[0]),
        pltpu.make_async_copy(edge_ref.at[pl.ds(tiles, tiles)], grad_ref.at[pl.ds(0, tiles)], sem.at[1]),
        pltpu.make_async_copy(low_s, grad_ref.at[pl.ds(n // SUB - tiles, tiles)], sem.at[2]),
    ]
    copies[0].start()
    copies[1].start()
    for g in range(p.groups):
        lanes = pl.ds(g * SUB, SUB)
        state = lambda kind, l, t: st_ref[p.state[kind, l, t], lanes, :]
        grad = {}
        for l in reversed(range(L)):
            wt = [wb_ref[l * (K + 1) + k, lanes, :] for k in reversed(range(K))]
            low = n - (L - 1 - l) * R
            pre = {n + s: ret_ref[l * R + s, lanes, :] for s in range(R)}
            for t in range(low - R, n):
                pre[t] = grad[t] * state("d", l, t) if t >= low else state("g", l, t)
            grad = {t: conv(wt, [pre[t + k] for k in range(K)]) for t in range(low - R, n)}
        for i in range(p.top):
            t = n - p.top + i
            row = grad[t] if t in grad else state("grad", 0, t)
            low_s[i // SUB, pl.ds(g * SUB * SUB + i % SUB, SUB, stride=SUB), :] = row
    copies[2].start()
    for copy in copies:
        copy.wait()


def finish(p, mine_ref, theirs_ref, w_ref, b_ref):
    L, K = p.layers, p.taps
    size = L * (K + 1) * SUB
    for g in range(p.groups):
        for l in range(L):
            for rows, where in ((SUB * K, l * SUB * K), (SUB, L * SUB * K + l * SUB)):
                there = pl.ds(g * size + where, rows)
                total = mine_ref[there, :] + theirs_ref[there, :]
                if rows == SUB * K:
                    w_ref[pl.ds((l * p.cols + g * SUB) * K, rows), :] = total
                else:
                    for c in range(SUB):
                        at = (g * SUB + c) * LANES
                        b_ref[l : l + 1, at : at + LANES] = total[c : c + 1, :]


def shifted(array, axis, by):
    devices = lax.axis_size(axis)
    return lax.ppermute(array, axis, [(i, (i + by) % devices) for i in range(devices)])


def swapped(array, axis, bit):
    return lax.ppermute(array, axis, [(i, i ^ bit) for i in range(lax.axis_size(axis))])


def summed_but_one(array, axis):
    devices = lax.axis_size(axis)
    bits = [1 << i for i in range(devices.bit_length() - 1)]
    if len(bits) > 2:
        one, two = bits[:2]
        near = swapped(array, axis, one)
        far = swapped(array, axis, two)
        both = swapped(array, axis, one ^ two)
        array = (array + near) + (far + both)
        bits = bits[2:]
    for bit in bits[:-1]:
        array = array + swapped(array, axis, bit)
    return array, swapped(array, axis, bits[-1])


def tiled(a):
    n, width = a.shape
    return a.reshape(n // SUB, SUB, width // LANES, LANES).transpose(0, 2, 1, 3).reshape(n // SUB, -1, LANES)


def untiled(a, n, width):
    return a.reshape(n // SUB, width // LANES, SUB, LANES).transpose(0, 2, 1, 3).reshape(n, width)


def shards(inputs, conv_weight, conv_bias, cotangent):
    n, width = inputs.shape
    layers, taps = conv_weight.shape[:2]
    p = Plan(n, width, layers, taps)
    L, K, H, cols = layers, taps, p.halo, p.cols
    f32 = lambda *shape: jax.ShapeDtypeStruct(shape, jnp.float32)
    vmem, hbm = pl.BlockSpec(memory_space=pltpu.VMEM), pl.BlockSpec(memory_space=pltpu.HBM)

    shape = (n // SUB, cols * SUB, LANES)
    per_row = (n, cols, LANES)
    work = n * width
    cost = lambda flops: pl.CostEstimate(flops=flops * work, bytes_accessed=0, transcendentals=0)
    params = lambda mib: pltpu.CompilerParams(vmem_limit_bytes=mib << 20)
    x, ct = tiled(inputs), tiled(cotangent)
    weights = conv_weight.reshape(L, K, cols, LANES).transpose(0, 2, 1, 3).reshape(L * cols * K, LANES)

    M = p.late
    low, high = -(-M // SUB) * SUB, -(-(M + H) // SUB) * SUB
    spot = lax.broadcasted_iota(jnp.int32, (low + high, width), 0)
    rows = jnp.where(
        spot < low, jnp.pad(cotangent[n - low :], ((0, high), (0, 0))), inputs[n - low - high :]
    ).reshape(-1, cols, LANES)
    from_before = shifted(rows[low - M :], "seq", 1)

    out, grad, st, wb = pl.pallas_call(
        functools.partial(interior, p),
        out_shape=(f32(*shape), f32(*shape), f32(p.state_rows, cols, LANES), f32(L * (K + 1), cols, LANES)),
        in_specs=[vmem] * 4,
        out_specs=(hbm, hbm, vmem, vmem),
        scratch_shapes=[pltpu.VMEM(per_row, jnp.float32)] * (2 * L - 1)
        + [pltpu.VMEM(shape, jnp.float32)] * 2
        + [pltpu.SemaphoreType.DMA((3 * p.groups,))],
        compiler_params=params(24),
        cost_estimate=cost(90),
        name="interior",
    )(x, ct, weights, conv_bias.reshape(L, cols, LANES))

    keep = jnp.where(lax.axis_index("seq") == 0, 0.0, 1.0) * jnp.ones((SUB, LANES), jnp.float32)
    edge, ret, sums = pl.pallas_call(
        functools.partial(border, p),
        out_shape=(
            f32(2 * p.top // SUB, *shape[1:]),
            f32(H, cols, LANES),
            f32(L * (K + 1) * cols, LANES),
        ),
        in_specs=[vmem] * 4,
        out_specs=(vmem,) * 3,
        compiler_params=params(8),
        cost_estimate=cost(10),
        name="border",
    )(keep, st, wb, from_before)
    mine, theirs = summed_but_one(sums, "seq")
    returned = shifted(ret, "seq", -1)

    out, grad = pl.pallas_call(
        functools.partial(edges, p),
        out_shape=(f32(*shape), f32(*shape)),
        in_specs=[hbm, hbm] + [vmem] * 4,
        out_specs=(hbm, hbm),
        scratch_shapes=[
            pltpu.VMEM((p.top // SUB, *shape[1:]), jnp.float32),
            pltpu.SemaphoreType.DMA((3,)),
        ],
        input_output_aliases={0: 0, 1: 1},
        compiler_params=params(4),
        cost_estimate=cost(5),
        name="edges",
    )(out, grad, edge, st, wb, returned)

    w_sum, b_sum = pl.pallas_call(
        functools.partial(finish, p),
        out_shape=(f32(*weights.shape), f32(L, width)),
        in_specs=[vmem] * 2,
        out_specs=(vmem, vmem),
        compiler_params=params(4),
        cost_estimate=cost(5),
        name="finish",
    )(mine, theirs)
    return (
        untiled(out, n, width),
        untiled(grad, n, width),
        w_sum.reshape(L, cols, K, LANES).transpose(0, 2, 1, 3).reshape(L, K, width),
        b_sum,
    )


def solution(mesh):
    in_specs = (P("seq", "chan"), P(None, None, "chan"), P(None, "chan"), P("seq", "chan"))
    out_specs = (P("seq", "chan"), P("seq", "chan"), P(None, None, "chan"), P(None, "chan"))
    return jax.shard_map(shards, mesh=mesh, in_specs=in_specs, out_specs=out_specs, check_vma=False)
```

```python
import functools

import jax
import jax.numpy as jnp
from jax import lax
from jax.experimental import pallas as pl
from jax.experimental.pallas import tpu as pltpu
from jax.sharding import PartitionSpec as P


LANES = 128
SUB = 8
BLOCK = 16


class Plan:
    def __init__(self, n, width, layers, taps):
        self.n, self.width, self.layers, self.taps = n, width, layers, taps
        self.reach = taps - 1
        self.halo = layers * self.reach
        self.late = self.halo - self.reach
        self.cols = width // LANES
        self.groups = self.cols // SUB
        self.top = top = -(-self.halo // SUB) * SUB
        rows = []
        L, R, H = layers, self.reach, self.halo
        rows += [(kind, 0, t) for kind in ("x", "ct") for t in range(H)]
        for l in range(1, L):
            rows += [("a", l, t) for t in range(l * R, H)]
        for l in range(L - 1):
            rows += [("d", l, t) for t in range((l + 1) * R, H)]
            rows += [("d", l, t) for t in range(n - (L - 1 - l) * R, n)]
        for l in range(L):
            low = n - (L - 1 - l) * R
            rows += [("g", l, t) for t in range(H, H + R)]
            rows += [("g", l, t) for t in range(low - R, low)]
        rows += [("out", 0, t) for t in range(H, top)]
        rows += [("grad", 0, t) for t in range(H, top)]
        rows += [("grad", 0, t) for t in range(n - top, n - H)]
        self.state = {key: i for i, key in enumerate(rows)}
        self.acc = len(rows)
        self.state_rows = len(rows) + layers * (taps + 1)


def conv(weights, window):
    total = weights[0] * window[0]
    for k in range(1, len(window)):
        total = total + weights[k] * window[k]
    return total + weights[len(window)] if len(weights) > len(window) else total


def gate(h):
    u = jnp.tanh(h)
    v = 1.0 + u
    act = h * v
    return act, v + act * (1.0 - u)


def interior(p, x_ref, ct_ref, w_ref, b_ref, out_hbm, grad_hbm, st_ref, wb_ref, *scratch):
    L, R, H, K, n = p.layers, p.reach, p.halo, p.taps, p.n
    a_s, d_s = scratch[: L - 1], scratch[L - 1 : 2 * L - 1]
    out_s, grad_s, sem = scratch[2 * L - 1 :]
    blocks = n // BLOCK
    copies = []

    def send(src, dst, first, last, g, i):
        where = (pl.ds(first, last - first), pl.ds(g * SUB * SUB, SUB * SUB), slice(None))
        copies.append(pltpu.make_async_copy(src.at[where], dst.at[where], sem.at[i]))
        copies[-1].start()

    for l in range(L):
        for g in range(p.groups):
            for k in range(K):
                wb_ref[l * (K + 1) + k, g * SUB : (g + 1) * SUB, :] = 0.5 * w_ref[
                    pl.ds((l * p.cols + g * SUB) * K + k, SUB, stride=K), :
                ]
            wb_ref[l * (K + 1) + K, g * SUB : (g + 1) * SUB, :] = 0.5 * b_ref[l, g * SUB : (g + 1) * SUB, :]

    for g in range(p.groups):
        lanes = pl.ds(g * SUB, SUB)

        def tile(base, off):
            return (base // SUB + off // SUB, pl.ds(g * SUB * SUB + off % SUB, SUB, stride=SUB), slice(None))

        wb = [[wb_ref[l * (K + 1) + k, lanes, :] for k in range(K + 1)] for l in range(L)]

        def forward(base, windows, first):
            windows = [list(w) for w in windows]
            for off in range(BLOCK):
                act = x_ref[tile(base, off)]
                for l in range(L):
                    windows[l] = windows[l] + [act]
                    if first and off < (l + 1) * R:
                        break
                    act, d = gate(conv(wb[l], windows[l][-K:]))
                    d_s[l][base + off, lanes, :] = d
                    if l < L - 1:
                        a_s[l][base + off, lanes, :] = act
                    else:
                        out_s[tile(base, off)] = act
            return [w[-R:] for w in windows]

        windows = forward(0, [[]] * L, True)
        lax.fori_loop(
            1, blocks, lambda i, w: forward(pl.multiple_of(i * BLOCK, BLOCK), w, False), windows
        )
        send(out_s, out_hbm, p.top // SUB, n // SUB, g, 3 * g)

        wt = [[wb_ref[l * (K + 1) + k, lanes, :] for k in range(K)] for l in range(L)]

        def backward(base, gs, acc, stop, last):
            gs, acc = [list(v) for v in gs], [list(v) for v in acc]
            acts = {}

            def act_at(l, off):
                if (l, off) not in acts:
                    if l == 0:
                        if off >= 0:
                            acts[l, off] = x_ref[tile(base, off)]
                        else:
                            acts[l, off] = x_ref[tile(base - BLOCK, off + BLOCK)]
                    else:
                        acts[l, off] = a_s[l - 1][base + off, lanes, :]
                return acts[l, off]

            for off in reversed(range(stop, BLOCK)):
                grad = ct_ref[tile(base, off)]
                for l in reversed(range(L)):
                    pre = grad * d_s[l][base + off, lanes, :]
                    gs[l] = ([pre] + gs[l])[:K]
                    for k in range(K):
                        acc[l][k] = acc[l][k] + pre * act_at(l, off - R + k)
                    acc[l][K] = acc[l][K] + pre
                    key = ("g", l, base + off if last or stop else None)
                    if key in p.state:
                        st_ref[p.state[key], lanes, :] = pre
                    if last and base + off >= n - (L - l) * R:
                        break
                    grad = conv(wt[l][::-1], gs[l])
                else:
                    grad_s[tile(base, off)] = grad
            return [v[:R] for v in gs], acc

        zero = jnp.zeros((SUB, LANES), jnp.float32)
        gs, acc = [[]] * L, [[zero] * (K + 1)] * L
        gs, acc = backward(n - BLOCK, gs, acc, 0, True)

        gs, acc = lax.fori_loop(
            0,
            blocks - 2,
            lambda i, c: backward(pl.multiple_of((blocks - 2 - i) * BLOCK, BLOCK), *c, 0, False),
            (gs, acc),
        )
        send(grad_s, grad_hbm, BLOCK // SUB, (n - p.top) // SUB, g, 3 * g + 1)
        gs, acc = backward(0, gs, acc, H, False)
        for l in range(L):
            for k in range(K + 1):
                st_ref[p.acc + l * (K + 1) + k, lanes, :] = acc[l][k]
        for (kind, l, t), i in p.state.items():
            if kind == "a":
                st_ref[i, lanes, :] = a_s[l - 1][t, lanes, :]
            elif kind == "d":
                st_ref[i, lanes, :] = d_s[l][t, lanes, :]
            elif kind == "x":
                st_ref[i, lanes, :] = x_ref[tile(0, t)]
            elif kind == "ct":
                st_ref[i, lanes, :] = ct_ref[tile(0, t)]
            elif kind == "out":
                st_ref[i, lanes, :] = out_s[tile(0, t)]
            elif kind == "grad":
                st_ref[i, lanes, :] = grad_s[tile(0, t)]
    for copy in copies:
        copy.wait()


def border(p, keep_ref, st_ref, wb_ref, up_ref, edge_ref, ret_ref, sums_ref):
    L, R, H, K, M = p.layers, p.reach, p.halo, p.taps, p.late
    size = L * (K + 1) * SUB
    tiles = p.top // SUB
    keep = keep_ref[...]
    for g in range(p.groups):
        lanes = pl.ds(g * SUB, SUB)
        wb = [[wb_ref[l * (K + 1) + k, lanes, :] for k in range(K + 1)] for l in range(L)]
        wt = [w[:K][::-1] for w in wb]
        acc = [[st_ref[p.acc + l * (K + 1) + k, lanes, :] for k in range(K + 1)] for l in range(L)]
        state = lambda kind, l, t: st_ref[p.state[kind, l, t], lanes, :]

        def put(plane, t, value):
            where = (plane * tiles + t // SUB, pl.ds(g * SUB * SUB + t % SUB, SUB, stride=SUB), slice(None))
            edge_ref[where] = value

        act = [dict() for _ in range(L + 1)]
        kept = [dict() for _ in range(L + 1)]
        d = [dict() for _ in range(L)]
        for t in range(-M - H, H):
            act[0][t] = up_ref[up_ref.shape[0] + t, lanes, :] if t < 0 else state("x", 0, t)

        def past(l, t):
            rows = range(t - R, t + 1)
            if t < 0:
                return [act[l][s] for s in rows]
            return [kept[l][s] if s < 0 else act[l][s] for s in rows]

        for l in range(L):
            for t in range(-R, 0):
                kept[l][t] = act[l][t] * keep
            for t in range(-M - H + (l + 1) * R, (l + 1) * R):
                act[l + 1][t], d[l][t] = gate(conv(wb[l], past(l, t)))
            if l < L - 1:
                for t in range((l + 1) * R, H):
                    act[l + 1][t], d[l][t] = state("a", l + 1, t), state("d", l, t)
        for t in range(p.top):
            put(0, t, act[L][t] if t < H else state("out", 0, t))

        pre = [{t: state("g", l, t) for t in range(H, H + R)} for l in range(L)]
        for t in reversed(range(-M, H)):
            if t == -1:
                for l in range(L):
                    for s in range(R):
                        pre[l][s] = ret_ref[l * R + s, lanes, :]
            grad = up_ref[M + t, lanes, :] if t < 0 else state("ct", 0, t)
            for l in reversed(range(L)):
                pre[l][t] = grad * d[l][t]
                if 0 <= t < R:
                    ret_ref[l * R + t, lanes, :] = pre[l][t] * keep
                if t >= -(L - 1 - l) * R:
                    window = past(l, t)
                    for k in range(K):
                        acc[l][k] = acc[l][k] + pre[l][t] * window[k]
                    acc[l][K] = acc[l][K] + pre[l][t]
                if t >= 0 or l > 0:
                    grad = conv(wt[l], [pre[l][t + k] for k in range(K)])
            if t >= 0:
                put(1, t, grad)
        for t in range(H, p.top):
            put(1, t, state("grad", 0, t))

        for l in range(L):
            for k in range(K):
                sums_ref[pl.ds(g * size + l * SUB * K + k, SUB, stride=K), :] = 0.5 * acc[l][k]
            sums_ref[pl.ds(g * size + L * SUB * K + l * SUB, SUB), :] = 0.5 * acc[l][K]


def edges(p, out_in, grad_in, edge_ref, st_ref, wb_ref, ret_ref, out_ref, grad_ref, low_s, sem):
    tiles, L, R, K, n = p.top // SUB, p.layers, p.reach, p.taps, p.n
    copies = [
        pltpu.make_async_copy(edge_ref.at[pl.ds(0, tiles)], out_ref.at[pl.ds(0, tiles)], sem.at[0]),
        pltpu.make_async_copy(edge_ref.at[pl.ds(tiles, tiles)], grad_ref.at[pl.ds(0, tiles)], sem.at[1]),
        pltpu.make_async_copy(low_s, grad_ref.at[pl.ds(n // SUB - tiles, tiles)], sem.at[2]),
    ]
    copies[0].start()
    copies[1].start()
    for g in range(p.groups):
        lanes = pl.ds(g * SUB, SUB)
        state = lambda kind, l, t: st_ref[p.state[kind, l, t], lanes, :]
        grad = {}
        for l in reversed(range(L)):
            wt = [wb_ref[l * (K + 1) + k, lanes, :] for k in reversed(range(K))]
            low = n - (L - 1 - l) * R
            pre = {n + s: ret_ref[l * R + s, lanes, :] for s in range(R)}
            for t in range(low - R, n):
                pre[t] = grad[t] * state("d", l, t) if t >= low else state("g", l, t)
            grad = {t: conv(wt, [pre[t + k] for k in range(K)]) for t in range(low - R, n)}
        for i in range(p.top):
            t = n - p.top + i
            row = grad[t] if t in grad else state("grad", 0, t)
            low_s[i // SUB, pl.ds(g * SUB * SUB + i % SUB, SUB, stride=SUB), :] = row
    copies[2].start()
    for copy in copies:
        copy.wait()


def finish(p, mine_ref, theirs_ref, w_ref, b_ref):
    L, K = p.layers, p.taps
    size = L * (K + 1) * SUB
    for g in range(p.groups):
        for l in range(L):
            for rows, where in ((SUB * K, l * SUB * K), (SUB, L * SUB * K + l * SUB)):
                there = pl.ds(g * size + where, rows)
                total = mine_ref[there, :] + theirs_ref[there, :]
                if rows == SUB * K:
                    w_ref[pl.ds((l * p.cols + g * SUB) * K, rows), :] = total
                else:
                    for c in range(SUB):
                        at = (g * SUB + c) * LANES
                        b_ref[l : l + 1, at : at + LANES] = total[c : c + 1, :]


def shifted(array, axis, by):
    devices = lax.axis_size(axis)
    return lax.ppermute(array, axis, [(i, (i + by) % devices) for i in range(devices)])


def swapped(array, axis, bit):
    return lax.ppermute(array, axis, [(i, i ^ bit) for i in range(lax.axis_size(axis))])


def summed_but_one(array, axis):
    devices = lax.axis_size(axis)
    bits = [1 << i for i in range(devices.bit_length() - 1)]
    if len(bits) > 2:
        one, two = bits[:2]
        near = swapped(array, axis, one)
        far = swapped(array, axis, two)
        both = swapped(array, axis, one ^ two)
        array = (array + near) + (far + both)
        bits = bits[2:]
    for bit in bits[:-1]:
        array = array + swapped(array, axis, bit)
    return array, swapped(array, axis, bits[-1])


def tiled(a):
    n, width = a.shape
    return a.reshape(n // SUB, SUB, width // LANES, LANES).transpose(0, 2, 1, 3).reshape(n // SUB, -1, LANES)


def untiled(a, n, width):
    return a.reshape(n // SUB, width // LANES, SUB, LANES).transpose(0, 2, 1, 3).reshape(n, width)


def shards(inputs, conv_weight, conv_bias, cotangent):
    n, width = inputs.shape
    layers, taps = conv_weight.shape[:2]
    p = Plan(n, width, layers, taps)
    L, K, H, cols = layers, taps, p.halo, p.cols
    f32 = lambda *shape: jax.ShapeDtypeStruct(shape, jnp.float32)
    vmem, hbm = pl.BlockSpec(memory_space=pltpu.VMEM), pl.BlockSpec(memory_space=pltpu.HBM)

    shape = (n // SUB, cols * SUB, LANES)
    per_row = (n, cols, LANES)
    work = n * width
    cost = lambda flops: pl.CostEstimate(flops=flops * work, bytes_accessed=0, transcendentals=0)
    params = lambda mib: pltpu.CompilerParams(vmem_limit_bytes=mib << 20)
    x, ct = tiled(inputs), tiled(cotangent)
    weights = conv_weight.reshape(L, K, cols, LANES).transpose(0, 2, 1, 3).reshape(L * cols * K, LANES)

    M = p.late
    low, high = -(-M // SUB) * SUB, -(-(M + H) // SUB) * SUB
    skip = high - M - H
    spot = lax.broadcasted_iota(jnp.int32, (low + high, width), 0)
    rows = jnp.where(
        spot < low + skip, jnp.pad(cotangent[n - low :], ((skip, high - skip), (0, 0))), inputs[n - low - high :]
    ).reshape(-1, cols, LANES)
    from_before = shifted(rows[low + skip - M :], "seq", 1)

    out, grad, st, wb = pl.pallas_call(
        functools.partial(interior, p),
        out_shape=(f32(*shape), f32(*shape), f32(p.state_rows, cols, LANES), f32(L * (K + 1), cols, LANES)),
        in_specs=[vmem] * 4,
        out_specs=(hbm, hbm, vmem, vmem),
        scratch_shapes=[pltpu.VMEM(per_row, jnp.float32)] * (2 * L - 1)
        + [pltpu.VMEM(shape, jnp.float32)] * 2
        + [pltpu.SemaphoreType.DMA((3 * p.groups,))],
        compiler_params=params(24),
        cost_estimate=cost(90),
        name="interior",
    )(x, ct, weights, conv_bias.reshape(L, cols, LANES))

    keep = jnp.where(lax.axis_index("seq") == 0, 0.0, 1.0) * jnp.ones((SUB, LANES), jnp.float32)
    edge, ret, sums = pl.pallas_call(
        functools.partial(border, p),
        out_shape=(
            f32(2 * p.top // SUB, *shape[1:]),
            f32(H, cols, LANES),
            f32(L * (K + 1) * cols, LANES),
        ),
        in_specs=[vmem] * 4,
        out_specs=(vmem,) * 3,
        compiler_params=params(8),
        cost_estimate=cost(10),
        name="border",
    )(keep, st, wb, from_before)
    mine, theirs = summed_but_one(sums, "seq")
    size, wide = lax.axis_size("seq"), lax.axis_size("chan")
    hops = [(i * wide + c, (i - 1) % size * wide + (c ^ 1 if i == 0 and wide % 2 == 0 else c)) for i in range(size) for c in range(wide)]
    returned = lax.ppermute(ret, ("seq", "chan"), hops)

    out, grad = pl.pallas_call(
        functools.partial(edges, p),
        out_shape=(f32(*shape), f32(*shape)),
        in_specs=[hbm, hbm] + [vmem] * 4,
        out_specs=(hbm, hbm),
        scratch_shapes=[
            pltpu.VMEM((p.top // SUB, *shape[1:]), jnp.float32),
            pltpu.SemaphoreType.DMA((3,)),
        ],
        input_output_aliases={0: 0, 1: 1},
        compiler_params=params(4),
        cost_estimate=cost(5),
        name="edges",
    )(out, grad, edge, st, wb, returned)

    w_sum, b_sum = pl.pallas_call(
        functools.partial(finish, p),
        out_shape=(f32(*weights.shape), f32(L, width)),
        in_specs=[vmem] * 2,
        out_specs=(vmem, vmem),
        compiler_params=params(4),
        cost_estimate=cost(5),
        name="finish",
    )(mine, theirs)
    return (
        untiled(out, n, width),
        untiled(grad, n, width),
        w_sum.reshape(L, cols, K, LANES).transpose(0, 2, 1, 3).reshape(L, K, width),
        b_sum,
    )


def solution(mesh):
    in_specs = (P("seq", "chan"), P(None, None, "chan"), P(None, "chan"), P("seq", "chan"))
    out_specs = (P("seq", "chan"), P("seq", "chan"), P(None, None, "chan"), P(None, "chan"))
    return jax.shard_map(shards, mesh=mesh, in_specs=in_specs, out_specs=out_specs, check_vma=False)
```
